32 devices in a mesh: head: 4 (over y, core), seq: 8 (over z, x).
Axes of the slice: x: 2, y: 2, z: 4, core: 2. Of those that a mesh axis runs over, the one named last changes fastest.
Arguments:
- cached_keys: bfloat16 [8, 32768, 8, 128], P(None, 'seq', 'head'), may hold values from -6 to 6
- queries: bfloat16 [8, 64, 128], P('seq', 'head'), may hold values from -6 to 6
- seq_lengths: int32 [8], replicated, may hold values from 1 to 32768
Outputs:
- page_min: bfloat16 [8, 2048, 8, 128], P('seq', 'head')
- page_max: bfloat16 [8, 2048, 8, 128], P('seq', 'head')
- page_mean: float32 [8, 2048, 8, 128], P('seq', 'head')
- page_score: float32 [8, 64, 2048], P('seq', None, 'head')
The draws below stay inside these ranges and needn't reach their ends.
All inputs are finite; a program needn't handle non-finite values.
Results may differ from the reference program's by a relative error of at most 0.001.
Values may be sent and summed in bfloat16 or wider, within the bound.
A program may use at most 192 MiB of HBM per device.

```python
import jax
import jax.numpy as jnp
from jax import lax

KVH = 8
QH = 64
HD = 128
PAGE = 16
LEN = 32768
SEQS = 8


def plant(values, key, smallest, high):
    longest = values.shape.index(max(values.shape))
    spots = []
    for shift in (0, 1):
        where = [jax.random.randint(jax.random.fold_in(key, axis), (), 0, length) for axis, length in enumerate(values.shape)]
        where[longest] = (where[longest] + shift) % values.shape[longest]
        spots.append(tuple(where))
    return values.at[spots[0]].set(smallest).at[spots[1]].set(high)


def block_levels(rng, shape, pieces, smallest, largest):
    def one(dim, parts):
        draws = jax.random.uniform(jax.random.fold_in(jax.random.fold_in(rng, 6), dim), (parts,), jnp.float32, smallest / len(pieces), largest / len(pieces))
        return jnp.repeat(jnp.exp(draws), shape[dim] // parts).reshape((-1,) + (1,) * (len(shape) - dim - 1))

    level = one(*pieces[0])
    for cut in pieces[1:]:
        level = level * one(*cut)
    return level


def noise(rng, shape, scale, most, split=(), held_as=jnp.bfloat16):
    result = scale * jax.random.normal(rng, shape, jnp.float32)
    if split:
        result = result * block_levels(rng, shape, split, -0.22, 0.18)
    return jnp.clip(result, -most, most).astype(held_as)


def setup_inputs(seed: int = 0) -> dict:
    key_list = jax.random.split(jax.random.key(seed), 4)
    return {
        "cached_keys": noise(key_list[0], (SEQS, LEN, KVH, HD), 1.0, 6.0, ((1, 8), (2, 4))),
        "queries": noise(key_list[1], (SEQS, QH, HD), 1.0, 6.0, ((0, 8), (1, 4))),
        "seq_lengths": plant(jax.random.randint(key_list[2], (SEQS,), 1, LEN + 1), jax.random.fold_in(key_list[2], 1), 1, LEN).astype(jnp.int32),
    }


def page_bounds(block, start, limit):
    seq_count = block.shape[0]
    tokens = block.shape[1]
    position = start + jnp.arange(tokens, dtype=jnp.int32)
    live_token = (position[None, :] < limit[:, None])[:, :, None, None]
    shaped = (seq_count, tokens // PAGE, PAGE, block.shape[2], block.shape[3])
    top_value = jnp.array(jnp.inf, block.dtype)
    lower = jnp.min(jnp.where(live_token, block, top_value).reshape(shaped), axis=2)
    upper = jnp.max(jnp.where(live_token, block, -top_value).reshape(shaped), axis=2)
    key_sums = jnp.sum(jnp.where(live_token, block, jnp.zeros((), block.dtype)).reshape(shaped), axis=2, dtype=jnp.float32)
    page_start = start + PAGE * jnp.arange(tokens // PAGE, dtype=jnp.int32)
    page_live = (page_start[None, :] < limit[:, None])[:, :, None, None]
    zero_value = jnp.zeros((), block.dtype)
    lower = jnp.where(page_live, lower, zero_value)
    upper = jnp.where(page_live, upper, zero_value)
    return lower, upper, key_sums


def page_average(key_sums, start, limit):
    page_start = start + PAGE * jnp.arange(key_sums.shape[1], dtype=jnp.int32)
    counts = jnp.clip(limit[:, None] - page_start[None, :], 0, PAGE).astype(jnp.float32)
    return key_sums / jnp.maximum(counts, 1.0)[:, :, None, None]


def bound_scores(query, lower, upper):
    seq_count, heads, width = query.shape
    kv_heads = lower.shape[2]
    grouped = query.astype(jnp.float32).reshape(seq_count, kv_heads, heads // kv_heads, width)
    positive = jnp.maximum(grouped, 0.0)
    negative = jnp.minimum(grouped, 0.0)
    score = jnp.einsum("shgc,sphc->shgp", positive, upper.astype(jnp.float32), precision=lax.Precision.HIGHEST)
    score = score + jnp.einsum("shgc,sphc->shgp", negative, lower.astype(jnp.float32), precision=lax.Precision.HIGHEST)
    return score.reshape(seq_count, heads, lower.shape[1]) * (width ** -0.5)


def one_sequence(inputs):
    block, limit, query = inputs
    limit = limit.reshape(1)
    lower, upper, key_sums = page_bounds(block[None], jnp.int32(0), limit)
    average = page_average(key_sums, jnp.int32(0), limit)
    score = bound_scores(query[None], lower, upper)
    return lower[0], upper[0], average[0], score[0]


def reference(cached_keys, queries, seq_lengths):
    lower, upper, average, score = lax.map(one_sequence, (cached_keys, seq_lengths, queries))
    return (lower, upper, average, score)
```

```python
import functools

import jax
import jax.numpy as jnp
from jax import lax
from jax.experimental import pallas as pl
from jax.experimental.pallas import tpu as pltpu
from jax.sharding import PartitionSpec as P

PAGE = 16
SLOTS = 3
BLOCK = 128
UNIT = 128
MESH = pl.DeviceIdType.MESH
SPAN = 28.0
TOP = 32767.0


def page_kernel(
    seqs, heads, lengths, keys, query, low_in, high_in, mean, score,
    buf, low, high, code, code_in, query_in, low_wide, high_wide, query_wide,
    key_sem, send_sem, recv_sem, query_send, query_recv, query_own,
):
    head = lax.axis_index("head")
    seq = lax.axis_index("seq")
    ratio = seqs // heads
    pages = keys.shape[1]
    width = keys.shape[3]
    lanes = keys.shape[4]
    block = buf.shape[2]
    blocks = pages // block
    steps = seqs * blocks
    rows = block * width
    chunk = min(64, rows)
    owner = seq // ratio
    part = lax.rem(seq, ratio)
    mine = owner == head

    def dest_of(step):
        pairs = seqs // 2
        half = pairs // 2
        k = step // blocks
        pair = k // 2
        own = seq // 2
        lower = own < half
        place = jnp.where(lower, own, pairs - 1 - own)
        near = jnp.where(place < half // 2, pairs - 1 - pair, pair - half)
        other = jnp.where(pair < half, pairs - 1 - pair, near)
        return 2 * jnp.where(lower, other, pairs - 1 - other) + lax.rem(seq + k, 2)

    def fetch(step):
        slot = lax.rem(step, SLOTS)
        dest = dest_of(step)
        at = pl.ds(lax.rem(step, blocks) * block, block)
        for t in range(PAGE):
            pltpu.make_async_copy(keys.at[dest, at, t], buf.at[slot, t], key_sem.at[slot]).start()

    for step in range(min(SLOTS - 1, steps)):
        fetch(jnp.int32(step))

    barrier = pltpu.get_barrier_semaphore()

    def greet(i, carry):
        source_head = i // ratio
        source_seq = head * ratio + lax.rem(i, ratio)

        @pl.when(jnp.logical_or(source_head != head, source_seq != seq))
        def _():
            pl.semaphore_signal(barrier, inc=1, device_id=(source_head, source_seq), device_id_type=MESH)

        return carry

    lax.fori_loop(0, seqs, greet, 0)
    for i in range(1, heads):
        pl.semaphore_signal(barrier, inc=1, device_id=(lax.rem(head + i, heads), seq), device_id_type=MESH)

    own_query = pltpu.make_async_copy(query, query_in.at[head], query_own)
    own_query.start()

    def query_copy(i, target):
        return pltpu.make_async_remote_copy(
            src_ref=query, dst_ref=query_in.at[head], send_sem=query_send.at[i], recv_sem=query_recv.at[i],
            device_id=(target, seq), device_id_type=MESH,
        )

    trio = ((low, low_in), (high, high_in), (code, code_in))
    index = head * ratio + part

    def landing(step):
        return pl.ds(part * pages + lax.rem(step, blocks) * block, block)

    def remote(step, k):
        source, target = trio[k]
        return pltpu.make_async_remote_copy(
            src_ref=source.at[step],
            dst_ref=target.at[landing(step), head],
            send_sem=send_sem.at[step, k],
            recv_sem=recv_sem.at[index, lax.rem(step, blocks), k],
            device_id=(owner, dest_of(step)),
            device_id_type=MESH,
        )

    row = lax.broadcasted_iota(jnp.int32, (chunk, lanes), 0)
    token = ((row // width) * PAGE).astype(jnp.int16)
    live_token = (row // width) * PAGE

    def work(step, carry):
        @pl.when(step + SLOTS - 1 < steps)
        def _():
            fetch(step + SLOTS - 1)

        slot = lax.rem(step, SLOTS)
        dest = dest_of(step)
        pltpu.make_async_copy(buf.at[slot], buf.at[slot], key_sem.at[slot]).wait()
        flat = buf.at[slot].reshape(PAGE, rows, lanes)
        limit = lengths[dest] - (seq * pages + lax.rem(step, blocks) * block) * PAGE
        low_flat = low.at[step].reshape(rows, lanes)
        high_flat = high.at[step].reshape(rows, lanes)
        code_flat = code.at[step].reshape(rows, lanes)

        def piece(c, carry):
            at = pl.ds(pl.multiple_of(c * chunk, chunk), chunk)
            left = jnp.clip(limit - c * (chunk // width * PAGE), 0, chunk // width * PAGE)
            first = flat[0, at, :]
            small = first
            large = first
            zero = jnp.zeros((chunk, lanes), jnp.bfloat16)
            total = jnp.where(token < left.astype(jnp.int16), first, zero).astype(jnp.float32)
            for t in range(1, PAGE):
                x = flat[t, at, :]
                keep = token < (left - t).astype(jnp.int16)
                y = jnp.where(keep, x, first)
                small = jnp.minimum(small, y)
                large = jnp.maximum(large, y)
                total = total + jnp.where(keep, x, zero).astype(jnp.float32)
            live = live_token < left
            small = jnp.where(live, small.astype(jnp.float32), 0.0)
            large = jnp.where(live, large.astype(jnp.float32), 0.0)
            bound = jnp.maximum(jnp.abs(small), jnp.abs(large))
            share = jnp.abs(total) / (PAGE * jnp.where(bound > 0.0, bound, 1.0))
            level = jnp.log2(jnp.maximum(share, 1e-30)) * (TOP / SPAN) + TOP
            level = jnp.clip(level + 0.5, 0.0, TOP)
            level = jnp.where(total < 0.0, -level, level)
            low_flat[at, :] = small.astype(low.dtype)
            high_flat[at, :] = large.astype(high.dtype)
            code_flat[at, :] = level.astype(jnp.int32).astype(jnp.int16)
            return carry

        lax.fori_loop(0, rows // chunk, piece, 0)

        @pl.when(step == 0)
        def _():
            pl.semaphore_wait(barrier, seqs - jnp.where(mine, 1, 0) + heads - 1)

        itself = jnp.logical_and(mine, dest == seq)

        @pl.when(itself)
        def _():
            low_in[landing(step), head] = low[step]
            high_in[landing(step), head] = high[step]
            code_in[landing(step), head] = code[step]

        @pl.when(jnp.logical_not(itself))
        def _():
            for k in range(3):
                remote(step, k).start()

        return carry

    lax.fori_loop(0, steps, work, 0)

    for i in range(heads - 1):
        query_copy(i, lax.rem(head + i + 1, heads)).start()
    own_query.wait()
    for i in range(heads - 1):
        query_copy(i, lax.rem(head + i + 1, heads)).wait()

    kv_heads = heads * width
    owned = mean.shape[0]
    group = query_in.shape[0] * query_in.shape[1] // kv_heads
    query_wide[...] = query_in[...].reshape(query_wide.shape).astype(jnp.float32)
    unit = min(UNIT, owned)
    unit_rows = unit * kv_heads
    span = max(pages // unit, 1)
    each = unit // block
    slab = min(128, unit_rows)
    limit = lengths[seq] - head * owned * PAGE
    low_flat = low_in.reshape(owned * kv_heads, lanes)
    high_flat = high_in.reshape(owned * kv_heads, lanes)
    code_flat = code_in.reshape(owned * kv_heads, lanes)
    mean_flat = mean.reshape(owned * kv_heads, lanes)
    page = lax.broadcasted_iota(jnp.int32, (slab, lanes), 0) // kv_heads

    def finish(i, carry):
        u = i
        if pages >= unit:
            u = lax.rem(i // span + seq, ratio) * span + lax.rem(i, span)

        def arrive(j, carry):
            source_head = j // each
            place = u * each + lax.rem(j, each)
            source_part = place // blocks
            itself = jnp.logical_and(source_head == head, head * ratio + source_part == seq)

            @pl.when(jnp.logical_not(itself))
            def _():
                for k in range(3):
                    source, target = trio[k]
                    pltpu.make_async_remote_copy(
                        src_ref=source.at[0],
                        dst_ref=target.at[pl.ds(place * block, block), source_head],
                        send_sem=send_sem.at[0, k],
                        recv_sem=recv_sem.at[source_head * ratio + source_part, lax.rem(place, blocks), k],
                        device_id=(source_head, head * ratio + source_part),
                        device_id_type=MESH,
                    ).wait_recv()

            return carry

        lax.fori_loop(0, heads * each, arrive, 0)

        def decode(c, carry):
            inside = pl.ds(pl.multiple_of(c * slab, slab), slab)
            at = pl.ds(pl.multiple_of(u * unit_rows + c * slab, slab), slab)
            small = low_flat[at, :].astype(jnp.float32)
            large = high_flat[at, :].astype(jnp.float32)
            low_wide[inside, :] = small
            high_wide[inside, :] = large
            bound = jnp.maximum(jnp.abs(small), jnp.abs(large))
            level = code_flat[at, :].astype(jnp.int32).astype(jnp.float32)
            share = jnp.exp2((jnp.abs(level) - TOP) * (SPAN / TOP))
            total = jnp.where(level == 0.0, 0.0, share * (PAGE * bound))
            total = jnp.where(level < 0.0, -total, total)
            first = u * unit + c * (slab // kv_heads)
            count = jnp.clip(limit - (first + page) * PAGE, 1, PAGE).astype(jnp.float32)
            mean_flat[at, :] = total / count
            return carry

        lax.fori_loop(0, unit_rows // slab, decode, 0)
        dims = (((1,), (1,)), ((), ()))
        across = pl.ds(pl.multiple_of(u * unit, unit), unit)
        for kv in range(kv_heads):
            q = query_wide[kv * group:(kv + 1) * group, :]
            up = high_wide[pl.ds(kv, unit, stride=kv_heads), :].astype(jnp.bfloat16)
            down = low_wide[pl.ds(kv, unit, stride=kv_heads), :].astype(jnp.bfloat16)
            both = lax.dot_general(
                jnp.maximum(q, 0.0).astype(jnp.bfloat16), up, dims, preferred_element_type=jnp.float32
            ) + lax.dot_general(
                jnp.minimum(q, 0.0).astype(jnp.bfloat16), down, dims, preferred_element_type=jnp.float32
            )
            score[kv * group:(kv + 1) * group, across] = both * lanes ** (-0.5)
        return carry

    lax.fori_loop(0, owned // unit, finish, 0)

    def sent(step, carry):
        @pl.when(jnp.logical_not(jnp.logical_and(mine, dest_of(step) == seq)))
        def _():
            for k in range(3):
                remote(step, k).wait_send()

        return carry

    lax.fori_loop(0, steps, sent, 0)


def store_kernel(low, high, mean, score, low_out, high_out, mean_out, score_out, sem):
    pairs = ((mean, mean_out), (low, low_out), (high, high_out), (score, score_out))
    copies = [pltpu.make_async_copy(source, target, sem.at[k]) for k, (source, target) in enumerate(pairs)]
    for copy in copies:
        copy.start()
    for copy in copies:
        copy.wait()


def local_step(heads, seqs, cached_keys, queries, seq_lengths):
    seq_count, tokens, width, lanes = cached_keys.shape
    pages = tokens // PAGE
    owned = pages * seqs // heads
    local_q = queries.shape[1]
    kv_heads = heads * width
    count_q = heads * local_q
    block = min(BLOCK, pages)
    blocks = pages // block
    unit = min(UNIT, owned)
    keys = cached_keys.reshape(seq_count, pages, PAGE, width, lanes)
    vmem = pl.BlockSpec(memory_space=pltpu.VMEM)
    hbm = pl.BlockSpec(memory_space=pltpu.HBM)
    shape = (owned, heads, width, lanes)
    low, high, mean, score = pl.pallas_call(
        functools.partial(page_kernel, seqs, heads),
        out_shape=(
            pltpu.VMEM(shape, jnp.bfloat16),
            pltpu.VMEM(shape, jnp.bfloat16),
            pltpu.VMEM((owned, kv_heads, lanes), jnp.float32),
            pltpu.VMEM((count_q, owned), jnp.float32),
        ),
        in_specs=[pl.BlockSpec(memory_space=pltpu.SMEM), hbm, hbm],
        out_specs=(vmem,) * 4,
        scratch_shapes=[
            pltpu.VMEM((SLOTS, PAGE, block, width, lanes), jnp.bfloat16),
            pltpu.VMEM((seqs * blocks, block, width, lanes), jnp.bfloat16),
            pltpu.VMEM((seqs * blocks, block, width, lanes), jnp.bfloat16),
            pltpu.VMEM((seqs * blocks, block, width, lanes), jnp.int16),
            pltpu.VMEM(shape, jnp.int16),
            pltpu.VMEM((heads, local_q, lanes), jnp.bfloat16),
            pltpu.VMEM((unit * kv_heads, lanes), jnp.float32),
            pltpu.VMEM((unit * kv_heads, lanes), jnp.float32),
            pltpu.VMEM((count_q, lanes), jnp.float32),
            pltpu.SemaphoreType.DMA((SLOTS,)),
            pltpu.SemaphoreType.DMA((seqs * blocks, 3)),
            pltpu.SemaphoreType.DMA((seqs, blocks, 3)),
            pltpu.SemaphoreType.DMA((heads - 1,)),
            pltpu.SemaphoreType.DMA((heads - 1,)),
            pltpu.SemaphoreType.DMA,
        ],
        compiler_params=pltpu.CompilerParams(collective_id=0, has_side_effects=True, vmem_limit_bytes=24 << 20),
        name="page_exchange",
    )(
        pltpu.with_memory_space_constraint(seq_lengths, pltpu.HBM),
        pltpu.with_memory_space_constraint(keys, pltpu.HBM),
        pltpu.with_memory_space_constraint(queries.reshape(local_q, lanes), pltpu.HBM),
    )
    whole = (1, owned, kv_heads, lanes)
    return pl.pallas_call(
        store_kernel,
        out_shape=(
            jax.ShapeDtypeStruct(whole, jnp.bfloat16),
            jax.ShapeDtypeStruct(whole, jnp.bfloat16),
            jax.ShapeDtypeStruct(whole, jnp.float32),
            jax.ShapeDtypeStruct((1, count_q, owned), jnp.float32),
        ),
        in_specs=[vmem] * 4,
        out_specs=(hbm,) * 4,
        scratch_shapes=[pltpu.SemaphoreType.DMA((4,))],
        compiler_params=pltpu.CompilerParams(vmem_limit_bytes=16 << 20),
        name="page_store",
    )(low.reshape(whole), high.reshape(whole), mean.reshape(whole), score.reshape(1, count_q, owned))


def solution(mesh):
    return jax.shard_map(
        functools.partial(local_step, mesh.shape["head"], mesh.shape["seq"]),
        mesh=mesh,
        in_specs=(P(None, "seq", "head", None), P("seq", "head", None), P()),
        out_specs=(
            P("seq", "head", None, None),
            P("seq", "head", None, None),
            P("seq", "head", None, None),
            P("seq", None, "head"),
        ),
        check_vma=False,
    )
```

```python
import functools

import jax
import jax.numpy as jnp
from jax import lax
from jax.experimental import pallas as pl
from jax.experimental.pallas import tpu as pltpu
from jax.sharding import PartitionSpec as P

PAGE = 16
SLOTS = 3
BLOCK = 128
UNIT = 128
MESH = pl.DeviceIdType.MESH
SPAN = 28.0
TOP = 32767.0


def gather(p, op, rows):
    early = rows < 4
    middle = jnp.logical_and(rows >= 2, rows < 6)
    even = lax.rem(rows, 4) < 2
    first = op(jnp.where(early, p[0], p[2]), pltpu.roll(jnp.where(early, p[2], p[0]), 4, 0))
    second = op(jnp.where(middle, p[1], p[3]), pltpu.roll(jnp.where(middle, p[3], p[1]), 4, 0))
    return op(jnp.where(even, first, second), pltpu.roll(jnp.where(even, second, first), 6, 0))


def shrink(x, op):
    x = op(x[:16], x[16:]).astype(jnp.float32)
    return op(x[:8], x[8:])


def page_kernel(
    seqs, heads, lengths_hbm, keys, query, low_in, high_in, mean, score,
    lengths, buf, low, high, code, code_in, query_in, low_wide, high_wide, query_wide,
    key_sem, send_sem, recv_sem, query_send, query_recv, query_own, length_sem,
):
    head = lax.axis_index("head")
    seq = lax.axis_index("seq")
    ratio = seqs // heads
    pages = keys.shape[1]
    tall = keys.shape[2]
    width = tall // PAGE
    lanes = keys.shape[3]
    block = buf.shape[1]
    blocks = pages // block
    steps = seqs * blocks
    rows = block * width
    group = min(8, block)
    chunk = min(32, block)
    owner = seq // ratio
    part = lax.rem(seq, ratio)
    mine = owner == head

    barrier = pltpu.get_barrier_semaphore()

    def greet(i, carry):
        source_head = i // ratio
        source_seq = head * ratio + lax.rem(i, ratio)

        @pl.when(jnp.logical_or(source_head != head, source_seq != seq))
        def _():
            pl.semaphore_signal(barrier, inc=1, device_id=(source_head, source_seq), device_id_type=MESH)

        return carry

    lax.fori_loop(0, seqs, greet, 0)
    for i in range(1, heads):
        pl.semaphore_signal(barrier, inc=1, device_id=(lax.rem(head + i, heads), seq), device_id_type=MESH)

    def dest_of(step):
        pairs = seqs // 2
        half = pairs // 2
        k = step // blocks
        pair = k // 2
        own = seq // 2
        lower = own < half
        place = jnp.where(lower, own, pairs - 1 - own)
        near = jnp.where(place < half // 2, pairs - 1 - pair, pair - half)
        other = jnp.where(pair < half, pairs - 1 - pair, near)
        return 2 * jnp.where(lower, other, pairs - 1 - other) + lax.rem(seq + k, 2)

    def fetch(step):
        slot = lax.rem(step, SLOTS)
        at = pl.ds(lax.rem(step, blocks) * block, block)
        return pltpu.make_async_copy(keys.at[dest_of(step), at], buf.at[slot], key_sem.at[slot])

    own_lengths = pltpu.make_async_copy(lengths_hbm, lengths, length_sem)
    own_lengths.start()
    for step in range(min(SLOTS - 1, steps)):
        fetch(jnp.int32(step)).start()
    own_query = pltpu.make_async_copy(query, query_in.at[head], query_own)
    own_query.start()

    def query_copy(i, target):
        return pltpu.make_async_remote_copy(
            src_ref=query, dst_ref=query_in.at[head], send_sem=query_send.at[i], recv_sem=query_recv.at[i],
            device_id=(target, seq), device_id_type=MESH,
        )

    trio = ((low, low_in), (high, high_in), (code, code_in))
    index = head * ratio + part

    def landing(step):
        return pl.ds(pl.multiple_of((part * pages + lax.rem(step, blocks) * block) * width, rows), rows)

    def remote(step, k):
        source, target = trio[k]
        return pltpu.make_async_remote_copy(
            src_ref=source.at[step],
            dst_ref=target.at[head, landing(step)],
            send_sem=send_sem.at[step, k],
            recv_sem=recv_sem.at[index, lax.rem(step, blocks), k],
            device_id=(owner, dest_of(step)),
            device_id_type=MESH,
        )

    adder_row = lax.broadcasted_iota(jnp.int32, (group * width, group * tall), 0)
    adder_column = lax.broadcasted_iota(jnp.int32, (group * width, group * tall), 1)
    adder = jnp.logical_and(
        adder_row // width == adder_column // tall, lax.rem(adder_row, width) == lax.rem(adder_column, width)
    ).astype(jnp.bfloat16)
    adder_token = (adder_column // width).astype(jnp.int16)
    eight = lax.broadcasted_iota(jnp.int32, (8, lanes), 0)
    page_of = lax.broadcasted_iota(jnp.int32, (chunk * width, lanes), 0) // width
    token_of = (lax.broadcasted_iota(jnp.int32, (tall, lanes), 0) // width).astype(jnp.int16)
    above = jnp.full((tall, lanes), jnp.inf, jnp.bfloat16)
    own_lengths.wait()

    def work(step, carry):
        @pl.when(step + SLOTS - 1 < steps)
        def _():
            fetch(step + SLOTS - 1).start()

        slot = lax.rem(step, SLOTS)
        dest = dest_of(step)
        fetch(step).wait()
        limit = jnp.clip(lengths[dest] - (seq * pages + lax.rem(step, blocks) * block) * PAGE, 0, block * PAGE)

        def piece(c, carry):
            small, large, total = [], [], []
            for g in range(chunk // group):
                start = c * chunk + g * group
                left = limit - start * PAGE
                lows, highs = [], []
                for p in range(group):
                    x = buf[slot, start + p]
                    keep = token_of < jnp.clip(left - p * PAGE, 0, PAGE).astype(jnp.int16)
                    lows.append(shrink(jnp.where(keep, x, above), jnp.minimum))
                    highs.append(shrink(jnp.where(keep, x, -above), jnp.maximum))
                for p in range(0, group, 4):
                    small.append(gather(lows[p:p + 4], jnp.minimum, eight))
                    large.append(gather(highs[p:p + 4], jnp.maximum, eight))
                x = buf[slot, pl.ds(start, group)].reshape(group * tall, lanes)
                counted = adder_token < jnp.clip(left, 0, group * PAGE).astype(jnp.int16)
                weight = jnp.where(counted, adder, jnp.zeros_like(adder))
                total.append(jnp.dot(weight, x, preferred_element_type=jnp.float32))
            live = (page_of + c * chunk) * PAGE < limit
            small = jnp.where(live, jnp.concatenate(small, axis=0), 0.0)
            large = jnp.where(live, jnp.concatenate(large, axis=0), 0.0)
            total = jnp.concatenate(total, axis=0)
            bound = jnp.maximum(jnp.abs(small), jnp.abs(large))
            share = jnp.abs(total) / (PAGE * jnp.where(bound > 0.0, bound, 1.0))
            level = jnp.log2(jnp.maximum(share, 1e-30)) * (TOP / SPAN) + TOP
            level = jnp.clip(level + 0.5, 0.0, TOP)
            level = jnp.where(total < 0.0, -level, level)
            at = pl.ds(pl.multiple_of(c * chunk * width, chunk * width), chunk * width)
            low[step, at, :] = small.astype(low.dtype)
            high[step, at, :] = large.astype(high.dtype)
            code[step, at, :] = level.astype(jnp.int32).astype(jnp.int16)
            return carry

        lax.fori_loop(0, block // chunk, piece, 0)

        @pl.when(step == 0)
        def _():
            pl.semaphore_wait(barrier, seqs - jnp.where(mine, 1, 0) + heads - 1)

        itself = jnp.logical_and(mine, dest == seq)

        @pl.when(itself)
        def _():
            low_in[head, landing(step)] = low[step]
            high_in[head, landing(step)] = high[step]
            code_in[head, landing(step)] = code[step]

        @pl.when(jnp.logical_not(itself))
        def _():
            for k in range(3):
                remote(step, k).start()

        return carry

    lax.fori_loop(0, steps, work, 0)

    for i in range(heads - 1):
        query_copy(i, lax.rem(head + i + 1, heads)).start()
    own_query.wait()
    for i in range(heads - 1):
        query_copy(i, lax.rem(head + i + 1, heads)).wait()

    owned = pages * ratio
    shared = query_in.shape[1] // width
    query_wide[...] = query_in[...].reshape(query_wide.shape).astype(jnp.float32)
    unit = min(UNIT, owned)
    unit_rows = unit * width
    span = max(pages // unit, 1)
    each = unit // block
    slab = min(128, unit_rows)
    limit = lengths[seq] - head * owned * PAGE
    row_page = lax.broadcasted_iota(jnp.int32, (slab, lanes), 0) // width

    def finish(i, carry):
        u = i // heads
        source_head = lax.rem(i, heads)
        if pages >= unit:
            u = lax.rem(u // span + seq, ratio) * span + lax.rem(u, span)

        def arrive(j, carry):
            place = u * each + j
            source_part = place // blocks
            itself = jnp.logical_and(source_head == head, head * ratio + source_part == seq)

            @pl.when(jnp.logical_not(itself))
            def _():
                for k in range(3):
                    source, target = trio[k]
                    pltpu.make_async_remote_copy(
                        src_ref=source.at[0],
                        dst_ref=target.at[source_head, pl.ds(pl.multiple_of(place * rows, rows), rows)],
                        send_sem=send_sem.at[0, k],
                        recv_sem=recv_sem.at[source_head * ratio + source_part, lax.rem(place, blocks), k],
                        device_id=(source_head, head * ratio + source_part),
                        device_id_type=MESH,
                    ).wait_recv()

            return carry

        lax.fori_loop(0, each, arrive, 0)

        def decode(c, carry):
            inside = pl.ds(pl.multiple_of(c * slab, slab), slab)
            at = pl.ds(pl.multiple_of(u * unit_rows + c * slab, slab), slab)
            small = low_in[source_head, at, :].astype(jnp.float32)
            large = high_in[source_head, at, :].astype(jnp.float32)
            low_wide[inside, :] = small
            high_wide[inside, :] = large
            bound = jnp.maximum(jnp.abs(small), jnp.abs(large))
            level = code_in[source_head, at, :].astype(jnp.int32).astype(jnp.float32)
            share = jnp.exp2((jnp.abs(level) - TOP) * (SPAN / TOP))
            total = jnp.where(level == 0.0, 0.0, share * (PAGE * bound))
            total = jnp.where(level < 0.0, -total, total)
            first = u * unit + c * (slab // width)
            count = jnp.clip(limit - (first + row_page) * PAGE, 1, PAGE).astype(jnp.float32)
            mean[source_head, at, :] = total / count
            return carry

        lax.fori_loop(0, unit_rows // slab, decode, 0)
        dims = (((1,), (1,)), ((), ()))
        across = pl.ds(pl.multiple_of(u * unit, unit), unit)
        for j in range(width):
            at = pl.ds(pl.multiple_of((source_head * width + j) * shared, shared), shared)
            q = query_wide[at, :]
            up = high_wide[pl.ds(j, unit, stride=width), :].astype(jnp.bfloat16)
            down = low_wide[pl.ds(j, unit, stride=width), :].astype(jnp.bfloat16)
            both = lax.dot_general(
                jnp.maximum(q, 0.0).astype(jnp.bfloat16), up, dims, preferred_element_type=jnp.float32
            ) + lax.dot_general(
                jnp.minimum(q, 0.0).astype(jnp.bfloat16), down, dims, preferred_element_type=jnp.float32
            )
            score[at, across] = both * lanes ** (-0.5)
        return carry

    lax.fori_loop(0, owned // unit * heads, finish, 0)

    def sent(step, carry):
        @pl.when(jnp.logical_not(jnp.logical_and(mine, dest_of(step) == seq)))
        def _():
            for k in range(3):
                remote(step, k).wait_send()

        return carry

    lax.fori_loop(0, steps, sent, 0)


def store_kernel(low, high, mean, score, low_out, high_out, mean_out, score_out, sem):
    heads = low.shape[0]
    copies = []
    for k, (source, target) in enumerate(((mean, mean_out), (low, low_out), (high, high_out))):
        for head in range(heads):
            copies.append(pltpu.make_async_copy(source.at[head], target.at[:, head], sem.at[k, head]))
    copies.append(pltpu.make_async_copy(score, score_out, sem.at[3, 0]))
    for copy in copies:
        copy.start()
    for copy in copies:
        copy.wait()


def local_step(heads, seqs, cached_keys, queries, seq_lengths):
    seq_count, tokens, width, lanes = cached_keys.shape
    pages = tokens // PAGE
    owned = pages * seqs // heads
    local_q = queries.shape[1]
    kv_heads = heads * width
    count_q = heads * local_q
    block = min(BLOCK, pages)
    blocks = pages // block
    unit = min(UNIT, owned)
    tall = PAGE * width
    keys = cached_keys.reshape(seq_count, pages, tall, lanes)
    vmem = pl.BlockSpec(memory_space=pltpu.VMEM)
    hbm = pl.BlockSpec(memory_space=pltpu.HBM)
    shape = (heads, owned * width, lanes)
    sends = (seqs * blocks, block * width, lanes)
    low, high, mean, score = pl.pallas_call(
        functools.partial(page_kernel, seqs, heads),
        out_shape=(
            pltpu.VMEM(shape, jnp.bfloat16),
            pltpu.VMEM(shape, jnp.bfloat16),
            pltpu.VMEM(shape, jnp.float32),
            pltpu.VMEM((count_q, owned), jnp.float32),
        ),
        in_specs=[hbm] * 3,
        out_specs=(vmem,) * 4,
        scratch_shapes=[
            pltpu.SMEM((seq_count,), jnp.int32),
            pltpu.VMEM((SLOTS, block, tall, lanes), jnp.bfloat16),
            pltpu.VMEM(sends, jnp.bfloat16),
            pltpu.VMEM(sends, jnp.bfloat16),
            pltpu.VMEM(sends, jnp.int16),
            pltpu.VMEM(shape, jnp.int16),
            pltpu.VMEM((heads, local_q, lanes), jnp.bfloat16),
            pltpu.VMEM((unit * width, lanes), jnp.float32),
            pltpu.VMEM((unit * width, lanes), jnp.float32),
            pltpu.VMEM((count_q, lanes), jnp.float32),
            pltpu.SemaphoreType.DMA((SLOTS,)),
            pltpu.SemaphoreType.DMA((seqs * blocks, 3)),
            pltpu.SemaphoreType.DMA((seqs, blocks, 3)),
            pltpu.SemaphoreType.DMA((heads - 1,)),
            pltpu.SemaphoreType.DMA((heads - 1,)),
            pltpu.SemaphoreType.DMA,
            pltpu.SemaphoreType.DMA,
        ],
        compiler_params=pltpu.CompilerParams(collective_id=0, has_side_effects=True, vmem_limit_bytes=24 << 20),
        name="page_exchange",
    )(
        pltpu.with_memory_space_constraint(seq_lengths, pltpu.HBM),
        pltpu.with_memory_space_constraint(keys, pltpu.HBM),
        pltpu.with_memory_space_constraint(queries.reshape(local_q, lanes), pltpu.HBM),
    )
    split = (heads, owned, width, lanes)
    whole = (owned, heads, width, lanes)
    low, high, mean, score = pl.pallas_call(
        store_kernel,
        out_shape=(
            jax.ShapeDtypeStruct(whole, jnp.bfloat16),
            jax.ShapeDtypeStruct(whole, jnp.bfloat16),
            jax.ShapeDtypeStruct(whole, jnp.float32),
            jax.ShapeDtypeStruct((count_q, owned), jnp.float32),
        ),
        in_specs=[vmem] * 4,
        out_specs=(hbm,) * 4,
        scratch_shapes=[pltpu.SemaphoreType.DMA((4, heads))],
        compiler_params=pltpu.CompilerParams(vmem_limit_bytes=16 << 20),
        name="page_store",
    )(low.reshape(split), high.reshape(split), mean.reshape(split), score)
    final = (1, owned, kv_heads, lanes)
    return low.reshape(final), high.reshape(final), mean.reshape(final), score.reshape(1, count_q, owned)


def solution(mesh):
    return jax.shard_map(
        functools.partial(local_step, mesh.shape["head"], mesh.shape["seq"]),
        mesh=mesh,
        in_specs=(P(None, "seq", "head", None), P("seq", "head", None), P()),
        out_specs=(
            P("seq", "head", None, None),
            P("seq", "head", None, None),
            P("seq", "head", None, None),
            P("seq", None, "head"),
        ),
        check_vma=False,
    )
```

```python
import functools

import jax
import jax.numpy as jnp
from jax import lax
from jax.experimental import pallas as pl
from jax.experimental.pallas import tpu as pltpu
from jax.sharding import PartitionSpec as P

PAGE = 16
SLOTS = 3
BLOCK = 128
UNIT = 128
MESH = pl.DeviceIdType.MESH
SPAN = 28.0
TOP = 32767.0


def gather(p, op, rows):
    early = rows < 4
    middle = jnp.logical_and(rows >= 2, rows < 6)
    even = lax.rem(rows, 4) < 2
    first = op(jnp.where(early, p[0], p[2]), pltpu.roll(jnp.where(early, p[2], p[0]), 4, 0))
    second = op(jnp.where(middle, p[1], p[3]), pltpu.roll(jnp.where(middle, p[3], p[1]), 4, 0))
    return op(jnp.where(even, first, second), pltpu.roll(jnp.where(even, second, first), 6, 0))


def shrink(x, op):
    x = op(x[:16], x[16:]).astype(jnp.float32)
    return op(x[:8], x[8:])


def page_kernel(
    seqs, heads, lengths_hbm, keys, query, low_in, high_in, mean, score,
    lengths, buf, low, high, code, code_in, query_in, low_wide, high_wide, query_wide,
    key_sem, send_sem, recv_sem, query_send, query_recv, query_own, length_sem,
):
    head = lax.axis_index("head")
    seq = lax.axis_index("seq")
    ratio = seqs // heads
    pages = keys.shape[1]
    tall = keys.shape[2]
    width = tall // PAGE
    lanes = keys.shape[3]
    block = buf.shape[1]
    blocks = pages // block
    steps = seqs * blocks
    rows = block * width
    group = min(8, block)
    chunk = min(32, block)
    owner = seq // ratio
    part = lax.rem(seq, ratio)
    mine = owner == head

    barrier = pltpu.get_barrier_semaphore()

    def greet(i, carry):
        source_head = i // ratio
        source_seq = head * ratio + lax.rem(i, ratio)

        @pl.when(jnp.logical_or(source_head != head, source_seq != seq))
        def _():
            pl.semaphore_signal(barrier, inc=1, device_id=(source_head, source_seq), device_id_type=MESH)

        return carry

    lax.fori_loop(0, seqs, greet, 0)
    for i in range(1, heads):
        pl.semaphore_signal(barrier, inc=1, device_id=(lax.rem(head + i, heads), seq), device_id_type=MESH)

    def dest_of(step):
        pairs = seqs // 2
        half = pairs // 2
        k = step // blocks
        pair = k // 2
        own = seq // 2
        lower = own < half
        place = jnp.where(lower, own, pairs - 1 - own)
        near = jnp.where(place < half // 2, pairs - 1 - pair, pair - half)
        other = jnp.where(pair < half, pairs - 1 - pair, near)
        return 2 * jnp.where(lower, other, pairs - 1 - other) + lax.rem(seq + k, 2)

    def fetch(step):
        slot = lax.rem(step, SLOTS)
        at = pl.ds(lax.rem(step, blocks) * block, block)
        return pltpu.make_async_copy(keys.at[dest_of(step), at], buf.at[slot], key_sem.at[slot])

    own_lengths = pltpu.make_async_copy(lengths_hbm, lengths, length_sem)
    own_lengths.start()
    for step in range(min(SLOTS - 1, steps)):
        fetch(jnp.int32(step)).start()
    own_query = pltpu.make_async_copy(query, query_in.at[head], query_own)
    own_query.start()

    def query_copy(i, target):
        return pltpu.make_async_remote_copy(
            src_ref=query, dst_ref=query_in.at[head], send_sem=query_send.at[i], recv_sem=query_recv.at[i],
            device_id=(target, seq), device_id_type=MESH,
        )

    trio = ((low, low_in), (high, high_in), (code, code_in))
    index = head * ratio + part

    def landing(step):
        return pl.ds(pl.multiple_of((part * pages + lax.rem(step, blocks) * block) * width, rows), rows)

    def remote(step, k):
        source, target = trio[k]
        return pltpu.make_async_remote_copy(
            src_ref=source.at[step],
            dst_ref=target.at[head, landing(step)],
            send_sem=send_sem.at[step, k],
            recv_sem=recv_sem.at[index, lax.rem(step, blocks), k],
            device_id=(owner, dest_of(step)),
            device_id_type=MESH,
        )

    adder_row = lax.broadcasted_iota(jnp.int32, (group * width, group * tall), 0)
    adder_column = lax.broadcasted_iota(jnp.int32, (group * width, group * tall), 1)
    adder = jnp.logical_and(
        adder_row // width == adder_column // tall, lax.rem(adder_row, width) == lax.rem(adder_column, width)
    ).astype(jnp.bfloat16)
    adder_token = (adder_column // width).astype(jnp.int16)
    eight = lax.broadcasted_iota(jnp.int32, (8, lanes), 0)
    page_of = lax.broadcasted_iota(jnp.int32, (chunk * width, lanes), 0) // width
    token_of = (lax.broadcasted_iota(jnp.int32, (tall, lanes), 0) // width).astype(jnp.int16)
    above = jnp.full((tall, lanes), jnp.inf, jnp.bfloat16)
    own_lengths.wait()

    def work(step, carry):
        @pl.when(step + SLOTS - 1 < steps)
        def _():
            fetch(step + SLOTS - 1).start()

        slot = lax.rem(step, SLOTS)
        dest = dest_of(step)
        fetch(step).wait()
        limit = jnp.clip(lengths[dest] - (seq * pages + lax.rem(step, blocks) * block) * PAGE, 0, block * PAGE)

        def piece(c, carry):
            small, large, total = [], [], []
            for g in range(chunk // group):
                start = c * chunk + g * group
                left = limit - start * PAGE
                lows, highs = [], []
                for p in range(group):
                    x = buf[slot, start + p]
                    keep = token_of < jnp.clip(left - p * PAGE, 0, PAGE).astype(jnp.int16)
                    lows.append(shrink(jnp.where(keep, x, above), jnp.minimum))
                    highs.append(shrink(jnp.where(keep, x, -above), jnp.maximum))
                for p in range(0, group, 4):
                    small.append(gather(lows[p:p + 4], jnp.minimum, eight))
                    large.append(gather(highs[p:p + 4], jnp.maximum, eight))
                x = buf[slot, pl.ds(start, group)].reshape(group * tall, lanes)
                counted = adder_token < jnp.clip(left, 0, group * PAGE).astype(jnp.int16)
                weight = jnp.where(counted, adder, jnp.zeros_like(adder))
                total.append(jnp.dot(weight, x, preferred_element_type=jnp.float32))
            live = (page_of + c * chunk) * PAGE < limit
            small = jnp.where(live, jnp.concatenate(small, axis=0), 0.0)
            large = jnp.where(live, jnp.concatenate(large, axis=0), 0.0)
            total = jnp.concatenate(total, axis=0)
            bound = jnp.maximum(jnp.abs(small), jnp.abs(large))
            share = jnp.abs(total) / (PAGE * jnp.where(bound > 0.0, bound, 1.0))
            level = jnp.log2(jnp.maximum(share, 1e-30)) * (TOP / SPAN) + TOP
            level = jnp.clip(level + 0.5, 0.0, TOP)
            level = jnp.where(total < 0.0, -level, level)
            at = pl.ds(pl.multiple_of(c * chunk * width, chunk * width), chunk * width)
            low[step, at, :] = small.astype(low.dtype)
            high[step, at, :] = large.astype(high.dtype)
            code[step, at, :] = level.astype(jnp.int32).astype(jnp.int16)
            return carry

        lax.fori_loop(0, block // chunk, piece, 0)

        @pl.when(step == 0)
        def _():
            pl.semaphore_wait(barrier, seqs - jnp.where(mine, 1, 0) + heads - 1)

        itself = jnp.logical_and(mine, dest == seq)

        @pl.when(itself)
        def _():
            low_in[head, landing(step)] = low[step]
            high_in[head, landing(step)] = high[step]
            code_in[head, landing(step)] = code[step]

        @pl.when(jnp.logical_not(itself))
        def _():
            for k in range(3):
                remote(step, k).start()

        return carry

    lax.fori_loop(0, steps, work, 0)

    for i in range(heads - 1):
        query_copy(i, lax.rem(head + i + 1, heads)).start()
    own_query.wait()
    for i in range(heads - 1):
        query_copy(i, lax.rem(head + i + 1, heads)).wait()

    owned = pages * ratio
    shared = query_in.shape[1] // width
    query_wide[...] = query_in[...].reshape(query_wide.shape).astype(jnp.float32)
    unit = min(UNIT, owned)
    unit_rows = unit * width
    span = max(pages // unit, 1)
    each = unit // block
    slab = min(128, unit_rows)
    limit = lengths[seq] - head * owned * PAGE
    row_page = lax.broadcasted_iota(jnp.int32, (slab, lanes), 0) // width

    dims = (((1,), (1,)), ((), ()))

    def arrived(u, source_head, kinds):
        def arrive(j, carry):
            place = u * each + j
            source_part = place // blocks
            itself = jnp.logical_and(source_head == head, head * ratio + source_part == seq)

            @pl.when(jnp.logical_not(itself))
            def _():
                for k in kinds:
                    source, target = trio[k]
                    pltpu.make_async_remote_copy(
                        src_ref=source.at[0],
                        dst_ref=target.at[source_head, pl.ds(pl.multiple_of(place * rows, rows), rows)],
                        send_sem=send_sem.at[0, k],
                        recv_sem=recv_sem.at[source_head * ratio + source_part, lax.rem(place, blocks), k],
                        device_id=(source_head, head * ratio + source_part),
                        device_id_type=MESH,
                    ).wait_recv()

            return carry

        lax.fori_loop(0, each, arrive, 0)

    def finish(i, carry):
        u = i
        if pages >= unit:
            u = lax.rem(i // span + seq, ratio) * span + lax.rem(i, span)
        across = pl.ds(pl.multiple_of(u * unit, unit), unit)

        def place_of(c):
            return pl.ds(pl.multiple_of(u * unit_rows + c * slab, slab), slab)

        def bounds(source_head, carry):
            arrived(u, source_head, (0, 1))

            def widen(c, carry):
                inside = pl.ds(pl.multiple_of(c * slab, slab), slab)
                at = place_of(c)
                small = low_in[source_head, at, :].astype(jnp.float32)
                large = high_in[source_head, at, :].astype(jnp.float32)
                low_wide[inside, :] = small
                high_wide[inside, :] = large
                first = u * unit + c * (slab // width)
                count = jnp.clip(limit - (first + row_page) * PAGE, 1, PAGE).astype(jnp.float32)
                mean[source_head, at, :] = jnp.maximum(jnp.abs(small), jnp.abs(large)) * PAGE / count
                return carry

            lax.fori_loop(0, unit_rows // slab, widen, 0)
            for j in range(width):
                at = pl.ds(pl.multiple_of((source_head * width + j) * shared, shared), shared)
                q = query_wide[at, :]
                up = high_wide[pl.ds(j, unit, stride=width), :].astype(jnp.bfloat16)
                down = low_wide[pl.ds(j, unit, stride=width), :].astype(jnp.bfloat16)
                both = lax.dot_general(
                    jnp.maximum(q, 0.0).astype(jnp.bfloat16), up, dims, preferred_element_type=jnp.float32
                ) + lax.dot_general(
                    jnp.minimum(q, 0.0).astype(jnp.bfloat16), down, dims, preferred_element_type=jnp.float32
                )
                score[at, across] = both * lanes ** (-0.5)
            return carry

        def means(source_head, carry):
            arrived(u, source_head, (2,))

            def decode(c, carry):
                at = place_of(c)
                level = code_in[source_head, at, :].astype(jnp.int32).astype(jnp.float32)
                share = jnp.exp2((jnp.abs(level) - TOP) * (SPAN / TOP))
                share = jnp.where(level == 0.0, 0.0, jnp.where(level < 0.0, -share, share))
                mean[source_head, at, :] = mean[source_head, at, :] * share
                return carry

            lax.fori_loop(0, unit_rows // slab, decode, 0)
            return carry

        lax.fori_loop(0, heads, bounds, 0)
        lax.fori_loop(0, heads, means, 0)
        return carry

    lax.fori_loop(0, owned // unit, finish, 0)

    def sent(step, carry):
        @pl.when(jnp.logical_not(jnp.logical_and(mine, dest_of(step) == seq)))
        def _():
            for k in range(3):
                remote(step, k).wait_send()

        return carry

    lax.fori_loop(0, steps, sent, 0)


def store_kernel(low, high, mean, score, low_out, high_out, mean_out, score_out, sem):
    heads = low.shape[0]
    copies = []
    for k, (source, target) in enumerate(((mean, mean_out), (low, low_out), (high, high_out))):
        for head in range(heads):
            copies.append(pltpu.make_async_copy(source.at[head], target.at[:, head], sem.at[k, head]))
    copies.append(pltpu.make_async_copy(score, score_out, sem.at[3, 0]))
    for copy in copies:
        copy.start()
    for copy in copies:
        copy.wait()


def local_step(heads, seqs, cached_keys, queries, seq_lengths):
    seq_count, tokens, width, lanes = cached_keys.shape
    pages = tokens // PAGE
    owned = pages * seqs // heads
    local_q = queries.shape[1]
    kv_heads = heads * width
    count_q = heads * local_q
    block = min(BLOCK, pages)
    blocks = pages // block
    unit = min(UNIT, owned)
    tall = PAGE * width
    keys = cached_keys.reshape(seq_count, pages, tall, lanes)
    vmem = pl.BlockSpec(memory_space=pltpu.VMEM)
    hbm = pl.BlockSpec(memory_space=pltpu.HBM)
    shape = (heads, owned * width, lanes)
    sends = (seqs * blocks, block * width, lanes)
    low, high, mean, score = pl.pallas_call(
        functools.partial(page_kernel, seqs, heads),
        out_shape=(
            pltpu.VMEM(shape, jnp.bfloat16),
            pltpu.VMEM(shape, jnp.bfloat16),
            pltpu.VMEM(shape, jnp.float32),
            pltpu.VMEM((count_q, owned), jnp.float32),
        ),
        in_specs=[hbm] * 3,
        out_specs=(vmem,) * 4,
        scratch_shapes=[
            pltpu.SMEM((seq_count,), jnp.int32),
            pltpu.VMEM((SLOTS, block, tall, lanes), jnp.bfloat16),
            pltpu.VMEM(sends, jnp.bfloat16),
            pltpu.VMEM(sends, jnp.bfloat16),
            pltpu.VMEM(sends, jnp.int16),
            pltpu.VMEM(shape, jnp.int16),
            pltpu.VMEM((heads, local_q, lanes), jnp.bfloat16),
            pltpu.VMEM((unit * width, lanes), jnp.float32),
            pltpu.VMEM((unit * width, lanes), jnp.float32),
            pltpu.VMEM((count_q, lanes), jnp.float32),
            pltpu.SemaphoreType.DMA((SLOTS,)),
            pltpu.SemaphoreType.DMA((seqs * blocks, 3)),
            pltpu.SemaphoreType.DMA((seqs, blocks, 3)),
            pltpu.SemaphoreType.DMA((heads - 1,)),
            pltpu.SemaphoreType.DMA((heads - 1,)),
            pltpu.SemaphoreType.DMA,
            pltpu.SemaphoreType.DMA,
        ],
        compiler_params=pltpu.CompilerParams(collective_id=0, has_side_effects=True, vmem_limit_bytes=24 << 20),
        name="page_exchange",
    )(
        pltpu.with_memory_space_constraint(seq_lengths, pltpu.HBM),
        pltpu.with_memory_space_constraint(keys, pltpu.HBM),
        pltpu.with_memory_space_constraint(queries.reshape(local_q, lanes), pltpu.HBM),
    )
    split = (heads, owned, width, lanes)
    whole = (owned, heads, width, lanes)
    low, high, mean, score = pl.pallas_call(
        store_kernel,
        out_shape=(
            jax.ShapeDtypeStruct(whole, jnp.bfloat16),
            jax.ShapeDtypeStruct(whole, jnp.bfloat16),
            jax.ShapeDtypeStruct(whole, jnp.float32),
            jax.ShapeDtypeStruct((count_q, owned), jnp.float32),
        ),
        in_specs=[vmem] * 4,
        out_specs=(hbm,) * 4,
        scratch_shapes=[pltpu.SemaphoreType.DMA((4, heads))],
        compiler_params=pltpu.CompilerParams(vmem_limit_bytes=16 << 20),
        name="page_store",
    )(low.reshape(split), high.reshape(split), mean.reshape(split), score)
    final = (1, owned, kv_heads, lanes)
    return low.reshape(final), high.reshape(final), mean.reshape(final), score.reshape(1, count_q, owned)


def solution(mesh):
    return jax.shard_map(
        functools.partial(local_step, mesh.shape["head"], mesh.shape["seq"]),
        mesh=mesh,
        in_specs=(P(None, "seq", "head", None), P("seq", "head", None), P()),
        out_specs=(
            P("seq", "head", None, None),
            P("seq", "head", None, None),
            P("seq", "head", None, None),
            P("seq", None, "head"),
        ),
        check_vma=False,
    )
```

```python
import functools

import jax
import jax.numpy as jnp
from jax import lax
from jax.experimental import pallas as pl
from jax.experimental.pallas import tpu as pltpu
from jax.sharding import PartitionSpec as P

PAGE = 16
SLOTS = 3
BLOCK = 128
LANE = 128
MESH = pl.DeviceIdType.MESH
SPAN = 28.0
TOP = 32767.0


def gather(p, op, rows):
    early = rows < 4
    middle = jnp.logical_and(rows >= 2, rows < 6)
    even = lax.rem(rows, 4) < 2
    first = op(jnp.where(early, p[0], p[2]), pltpu.roll(jnp.where(early, p[2], p[0]), 4, 0))
    second = op(jnp.where(middle, p[1], p[3]), pltpu.roll(jnp.where(middle, p[3], p[1]), 4, 0))
    return op(jnp.where(even, first, second), pltpu.roll(jnp.where(even, second, first), 6, 0))


def shrink(x, op):
    x = op(x[:16], x[16:]).astype(jnp.float32)
    return op(x[:8], x[8:])


def page_kernel(
    seqs, heads, lengths_hbm, keys, query, bounds_in, mean, score,
    lengths, buf, bounds, code, code_in, query_in, low_wide, high_wide, query_wide,
    key_sem, bounds_send, bounds_recv, code_send, code_recv, query_send, query_recv, query_own, length_sem,
):
    head = lax.axis_index("head")
    seq = lax.axis_index("seq")
    ratio = seqs // heads
    pages = keys.shape[1]
    tall = keys.shape[2]
    width = tall // PAGE
    lanes = keys.shape[3]
    block = buf.shape[1]
    blocks = pages // block
    steps = seqs * blocks
    rows = block * width
    group = min(8, block)
    chunk = min(32, block)
    owner = seq // ratio
    part = lax.rem(seq, ratio)
    mine = owner == head

    barrier = pltpu.get_barrier_semaphore()

    def greet(i, carry):
        source_head = i // ratio
        source_seq = head * ratio + lax.rem(i, ratio)

        @pl.when(jnp.logical_or(source_head != head, source_seq != seq))
        def _():
            pl.semaphore_signal(barrier, inc=1, device_id=(source_head, source_seq), device_id_type=MESH)

        return carry

    lax.fori_loop(0, seqs, greet, 0)
    for i in range(1, heads):
        pl.semaphore_signal(barrier, inc=1, device_id=(lax.rem(head + i, heads), seq), device_id_type=MESH)

    def dest_of(step):
        pairs = seqs // 2
        half = pairs // 2
        k = step // blocks
        pair = k // 2
        own = seq // 2
        lower = own < half
        place = jnp.where(lower, own, pairs - 1 - own)
        near = jnp.where(place < half // 2, pairs - 1 - pair, pair - half)
        other = jnp.where(pair < half, pairs - 1 - pair, near)
        return 2 * jnp.where(lower, other, pairs - 1 - other) + lax.rem(seq + k, 2)

    def fetch(step):
        slot = lax.rem(step, SLOTS)
        at = pl.ds(lax.rem(step, blocks) * block, block)
        return pltpu.make_async_copy(keys.at[dest_of(step), at], buf.at[slot], key_sem.at[slot])

    own_lengths = pltpu.make_async_copy(lengths_hbm, lengths, length_sem)
    own_lengths.start()
    for step in range(min(SLOTS - 1, steps)):
        fetch(jnp.int32(step)).start()
    own_query = pltpu.make_async_copy(query, query_in.at[head], query_own)
    own_query.start()

    def query_copy(i, target):
        return pltpu.make_async_remote_copy(
            src_ref=query, dst_ref=query_in.at[head], send_sem=query_send.at[i], recv_sem=query_recv.at[i],
            device_id=(target, seq), device_id_type=MESH,
        )

    index = head * ratio + part

    def landing(step):
        return pl.ds(pl.multiple_of((part * pages + lax.rem(step, blocks) * block) * width, rows), rows)

    def inside_of(step):
        return pl.ds(pl.multiple_of(lax.rem(step, blocks) * rows, rows), rows)

    def whole_bounds(step):
        return pltpu.make_async_remote_copy(
            src_ref=bounds.at[step // blocks],
            dst_ref=bounds_in.at[head, part],
            send_sem=bounds_send.at[step // blocks],
            recv_sem=bounds_recv.at[index],
            device_id=(owner, dest_of(step)),
            device_id_type=MESH,
        )

    def block_bounds(step):
        return pltpu.make_async_remote_copy(
            src_ref=bounds.at[step // blocks, :, inside_of(step)],
            dst_ref=bounds_in.at[head, part, :, inside_of(step)],
            send_sem=bounds_send.at[step // blocks],
            recv_sem=bounds_recv.at[index],
            device_id=(owner, dest_of(step)),
            device_id_type=MESH,
        )

    def block_code(step):
        return pltpu.make_async_remote_copy(
            src_ref=code.at[step // blocks, inside_of(step)],
            dst_ref=code_in.at[head, landing(step)],
            send_sem=code_send.at[step],
            recv_sem=code_recv.at[index, lax.rem(step, blocks)],
            device_id=(owner, dest_of(step)),
            device_id_type=MESH,
        )

    adder_row = lax.broadcasted_iota(jnp.int32, (group * width, group * tall), 0)
    adder_column = lax.broadcasted_iota(jnp.int32, (group * width, group * tall), 1)
    adder = jnp.logical_and(
        adder_row // width == adder_column // tall, lax.rem(adder_row, width) == lax.rem(adder_column, width)
    ).astype(jnp.bfloat16)
    adder_token = (adder_column // width).astype(jnp.int16)
    eight = lax.broadcasted_iota(jnp.int32, (8, lanes), 0)
    page_of = lax.broadcasted_iota(jnp.int32, (chunk * width, lanes), 0) // width
    token_of = (lax.broadcasted_iota(jnp.int32, (tall, lanes), 0) // width).astype(jnp.int16)
    above = jnp.full((tall, lanes), jnp.inf, jnp.bfloat16)
    own_lengths.wait()

    def work(step, carry):
        @pl.when(step + SLOTS - 1 < steps)
        def _():
            fetch(step + SLOTS - 1).start()

        slot = lax.rem(step, SLOTS)
        dest = dest_of(step)
        fetch(step).wait()
        limit = jnp.clip(lengths[dest] - (seq * pages + lax.rem(step, blocks) * block) * PAGE, 0, block * PAGE)

        def piece(c, carry):
            small, large, total = [], [], []
            for g in range(chunk // group):
                start = c * chunk + g * group
                left = limit - start * PAGE
                lows, highs = [], []
                for p in range(group):
                    x = buf[slot, start + p]
                    keep = token_of < jnp.clip(left - p * PAGE, 0, PAGE).astype(jnp.int16)
                    lows.append(shrink(jnp.where(keep, x, above), jnp.minimum))
                    highs.append(shrink(jnp.where(keep, x, -above), jnp.maximum))
                for p in range(0, group, 4):
                    small.append(gather(lows[p:p + 4], jnp.minimum, eight))
                    large.append(gather(highs[p:p + 4], jnp.maximum, eight))
                x = buf[slot, pl.ds(start, group)].reshape(group * tall, lanes)
                counted = adder_token < jnp.clip(left, 0, group * PAGE).astype(jnp.int16)
                weight = jnp.where(counted, adder, jnp.zeros_like(adder))
                total.append(jnp.dot(weight, x, preferred_element_type=jnp.float32))
            live = (page_of + c * chunk) * PAGE < limit
            small = jnp.where(live, jnp.concatenate(small, axis=0), 0.0)
            large = jnp.where(live, jnp.concatenate(large, axis=0), 0.0)
            total = jnp.concatenate(total, axis=0)
            bound = jnp.maximum(jnp.abs(small), jnp.abs(large))
            share = jnp.abs(total) / (PAGE * jnp.where(bound > 0.0, bound, 1.0))
            level = jnp.log2(jnp.maximum(share, 1e-30)) * (TOP / SPAN) + TOP
            level = jnp.clip(level + 0.5, 0.0, TOP)
            level = jnp.where(total < 0.0, -level, level)
            at = pl.ds(pl.multiple_of(lax.rem(step, blocks) * rows + c * chunk * width, chunk * width), chunk * width)
            bounds[step // blocks, 0, at, :] = small.astype(bounds.dtype)
            bounds[step // blocks, 1, at, :] = large.astype(bounds.dtype)
            code[step // blocks, at, :] = level.astype(jnp.int32).astype(jnp.int16)
            return carry

        lax.fori_loop(0, block // chunk, piece, 0)

        @pl.when(step == 0)
        def _():
            pl.semaphore_wait(barrier, seqs - jnp.where(mine, 1, 0) + heads - 1)

        itself = jnp.logical_and(mine, dest == seq)

        @pl.when(itself)
        def _():
            bounds_in[head, part, :, inside_of(step)] = bounds[step // blocks, :, inside_of(step)]
            code_in[head, landing(step)] = code[step // blocks, inside_of(step)]

        @pl.when(jnp.logical_and(jnp.logical_not(itself), step < blocks))
        def _():
            block_bounds(step).start()
            block_code(step).start()

        complete = jnp.logical_and(step >= blocks, lax.rem(step, blocks) == blocks - 1)

        @pl.when(jnp.logical_and(jnp.logical_not(itself), complete))
        def _():
            whole_bounds(step).start()
            for b in range(blocks):
                block_code(step - (blocks - 1) + b).start()

        return carry

    lax.fori_loop(0, steps, work, 0)

    for i in range(heads - 1):
        query_copy(i, lax.rem(head + i + 1, heads)).start()
    own_query.wait()
    for i in range(heads - 1):
        query_copy(i, lax.rem(head + i + 1, heads)).wait()

    owned = pages * ratio
    shared = query_in.shape[1] // width
    query_wide[...] = query_in[...].reshape(query_wide.shape).astype(jnp.float32)
    unit = min(max(LANE, pages), owned)
    unit_rows = unit * width
    each = unit // pages
    message = pages * width
    slab = min(256, rows)
    parts = message // slab
    limit = lengths[seq] - head * owned * PAGE
    row_page = lax.broadcasted_iota(jnp.int32, (slab, lanes), 0) // width

    dims = (((1,), (1,)), ((), ()))

    def finish(i, carry):
        u = i
        if each == 1:
            u = lax.rem(i + seq, ratio)
        across = pl.ds(pl.multiple_of(u * unit, unit), unit)

        def elsewhere(source_head, source_part):
            return jnp.logical_or(source_head != head, head * ratio + source_part != seq)

        def spread(source_head, carry):
            for j in range(each):
                source_part = u * each + j

                @pl.when(elsewhere(source_head, source_part))
                def _():
                    pltpu.make_async_remote_copy(
                        src_ref=bounds.at[0],
                        dst_ref=bounds_in.at[source_head, source_part],
                        send_sem=bounds_send.at[0],
                        recv_sem=bounds_recv.at[source_head * ratio + source_part],
                        device_id=(source_head, head * ratio + source_part),
                        device_id_type=MESH,
                    ).wait_recv()

            def widen(c, carry):
                inside = pl.ds(pl.multiple_of(c * slab, slab), slab)
                at = pl.ds(pl.multiple_of(u * unit_rows + c * slab, slab), slab)
                local = pl.ds(pl.multiple_of(lax.rem(c, parts) * slab, slab), slab)
                small = bounds_in[source_head, u * each + c // parts, 0, local, :].astype(jnp.float32)
                large = bounds_in[source_head, u * each + c // parts, 1, local, :].astype(jnp.float32)
                low_wide[inside, :] = small
                high_wide[inside, :] = large
                first = u * unit + c * (slab // width)
                count = jnp.clip(limit - (first + row_page) * PAGE, 1, PAGE).astype(jnp.float32)
                mean[source_head, at, :] = jnp.maximum(jnp.abs(small), jnp.abs(large)) * PAGE / count
                return carry

            lax.fori_loop(0, unit_rows // slab, widen, 0)
            for j in range(width):
                at = pl.ds(pl.multiple_of((source_head * width + j) * shared, shared), shared)
                q = query_wide[at, :]
                up = high_wide[pl.ds(j, unit, stride=width), :].astype(jnp.bfloat16)
                down = low_wide[pl.ds(j, unit, stride=width), :].astype(jnp.bfloat16)
                both = lax.dot_general(
                    jnp.maximum(q, 0.0).astype(jnp.bfloat16), up, dims, preferred_element_type=jnp.float32
                ) + lax.dot_general(
                    jnp.minimum(q, 0.0).astype(jnp.bfloat16), down, dims, preferred_element_type=jnp.float32
                )
                score[at, across] = both * lanes ** (-0.5)
            return carry

        def average(n, carry):
            source_head = lax.rem(n, heads)
            place = u * each * blocks + n // heads
            source_part = place // blocks

            @pl.when(elsewhere(source_head, source_part))
            def _():
                pltpu.make_async_remote_copy(
                    src_ref=code.at[0, pl.ds(0, rows)],
                    dst_ref=code_in.at[source_head, pl.ds(pl.multiple_of(place * rows, rows), rows)],
                    send_sem=code_send.at[0],
                    recv_sem=code_recv.at[source_head * ratio + source_part, lax.rem(place, blocks)],
                    device_id=(source_head, head * ratio + source_part),
                    device_id_type=MESH,
                ).wait_recv()

            def decode(c, carry):
                at = pl.ds(pl.multiple_of(place * rows + c * slab, slab), slab)
                level = code_in[source_head, at, :].astype(jnp.int32).astype(jnp.float32)
                share = jnp.exp2((jnp.abs(level) - TOP) * (SPAN / TOP))
                share = jnp.where(level == 0.0, 0.0, jnp.where(level < 0.0, -share, share))
                mean[source_head, at, :] = mean[source_head, at, :] * share
                return carry

            lax.fori_loop(0, rows // slab, decode, 0)
            return carry

        lax.fori_loop(0, heads, spread, 0)
        lax.fori_loop(0, heads * each * blocks, average, 0)
        return carry

    lax.fori_loop(0, owned // unit, finish, 0)

    def sent(step, carry):
        @pl.when(jnp.logical_not(jnp.logical_and(mine, dest_of(step) == seq)))
        def _():
            block_code(step).wait_send()

            @pl.when(lax.rem(step, blocks) == 0)
            def _():
                whole_bounds(step).wait_send()

        return carry

    lax.fori_loop(0, steps, sent, 0)


def store_kernel(bounds, mean, score, low_out, high_out, mean_out, score_out, sem):
    copies = []
    for head in range(bounds.shape[0]):
        copies.append(pltpu.make_async_copy(mean.at[head], mean_out.at[:, :, head], sem.at[0, head]))
        for k, target in ((0, low_out), (1, high_out)):
            copies.append(pltpu.make_async_copy(bounds.at[head, :, k], target.at[:, :, head], sem.at[1 + k, head]))
    copies.append(pltpu.make_async_copy(score, score_out, sem.at[3, 0]))
    for copy in copies:
        copy.start()
    for copy in copies:
        copy.wait()


def local_step(heads, seqs, cached_keys, queries, seq_lengths):
    seq_count, tokens, width, lanes = cached_keys.shape
    pages = tokens // PAGE
    owned = pages * seqs // heads
    local_q = queries.shape[1]
    kv_heads = heads * width
    count_q = heads * local_q
    block = min(BLOCK, pages)
    blocks = pages // block
    unit = min(max(LANE, pages), owned)
    tall = PAGE * width
    keys = cached_keys.reshape(seq_count, pages, tall, lanes)
    vmem = pl.BlockSpec(memory_space=pltpu.VMEM)
    hbm = pl.BlockSpec(memory_space=pltpu.HBM)
    shape = (heads, owned * width, lanes)
    ratio = seqs // heads
    message = pages * width
    bounds, mean, score = pl.pallas_call(
        functools.partial(page_kernel, seqs, heads),
        out_shape=(
            pltpu.VMEM((heads, ratio, 2, message, lanes), jnp.bfloat16),
            pltpu.VMEM(shape, jnp.float32),
            pltpu.VMEM((count_q, owned), jnp.float32),
        ),
        in_specs=[hbm] * 3,
        out_specs=(vmem,) * 3,
        scratch_shapes=[
            pltpu.SMEM((seq_count,), jnp.int32),
            pltpu.VMEM((SLOTS, block, tall, lanes), jnp.bfloat16),
            pltpu.VMEM((seqs, 2, message, lanes), jnp.bfloat16),
            pltpu.VMEM((seqs, message, lanes), jnp.int16),
            pltpu.VMEM(shape, jnp.int16),
            pltpu.VMEM((heads, local_q, lanes), jnp.bfloat16),
            pltpu.VMEM((unit * width, lanes), jnp.float32),
            pltpu.VMEM((unit * width, lanes), jnp.float32),
            pltpu.VMEM((count_q, lanes), jnp.float32),
            pltpu.SemaphoreType.DMA((SLOTS,)),
            pltpu.SemaphoreType.DMA((seqs,)),
            pltpu.SemaphoreType.DMA((seqs,)),
            pltpu.SemaphoreType.DMA((seqs * blocks,)),
            pltpu.SemaphoreType.DMA((seqs, blocks)),
            pltpu.SemaphoreType.DMA((heads - 1,)),
            pltpu.SemaphoreType.DMA((heads - 1,)),
            pltpu.SemaphoreType.DMA,
            pltpu.SemaphoreType.DMA,
        ],
        compiler_params=pltpu.CompilerParams(collective_id=0, has_side_effects=True, vmem_limit_bytes=24 << 20),
        name="page_exchange",
    )(
        pltpu.with_memory_space_constraint(seq_lengths, pltpu.HBM),
        pltpu.with_memory_space_constraint(keys, pltpu.HBM),
        pltpu.with_memory_space_constraint(queries.reshape(local_q, lanes), pltpu.HBM),
    )
    whole = (ratio, pages, heads, width, lanes)
    low, high, mean, score = pl.pallas_call(
        store_kernel,
        out_shape=(
            jax.ShapeDtypeStruct(whole, jnp.bfloat16),
            jax.ShapeDtypeStruct(whole, jnp.bfloat16),
            jax.ShapeDtypeStruct(whole, jnp.float32),
            jax.ShapeDtypeStruct((count_q, owned), jnp.float32),
        ),
        in_specs=[vmem] * 3,
        out_specs=(hbm,) * 4,
        scratch_shapes=[pltpu.SemaphoreType.DMA((4, heads))],
        compiler_params=pltpu.CompilerParams(vmem_limit_bytes=16 << 20),
        name="page_store",
    )(
        bounds.reshape(heads, ratio, 2, pages, width, lanes),
        mean.reshape(heads, ratio, pages, width, lanes),
        score,
    )
    final = (1, owned, kv_heads, lanes)
    return low.reshape(final), high.reshape(final), mean.reshape(final), score.reshape(1, count_q, owned)


def solution(mesh):
    return jax.shard_map(
        functools.partial(local_step, mesh.shape["head"], mesh.shape["seq"]),
        mesh=mesh,
        in_specs=(P(None, "seq", "head", None), P("seq", "head", None), P()),
        out_specs=(
            P("seq", "head", None, None),
            P("seq", "head", None, None),
            P("seq", "head", None, None),
            P("seq", None, "head"),
        ),
        check_vma=False,
    )
```

```python
import functools

import jax
import jax.numpy as jnp
from jax import lax
from jax.experimental import pallas as pl
from jax.experimental.pallas import tpu as pltpu
from jax.sharding import PartitionSpec as P

PAGE = 16
SLOTS = 3
BLOCK = 128
LANE = 128
MESH = pl.DeviceIdType.MESH
SPAN = 28.0
TOP = 32767.0


def gather(p, op, rows):
    early = rows < 4
    middle = jnp.logical_and(rows >= 2, rows < 6)
    even = lax.rem(rows, 4) < 2
    first = op(jnp.where(early, p[0], p[2]), pltpu.roll(jnp.where(early, p[2], p[0]), 4, 0))
    second = op(jnp.where(middle, p[1], p[3]), pltpu.roll(jnp.where(middle, p[3], p[1]), 4, 0))
    return op(jnp.where(even, first, second), pltpu.roll(jnp.where(even, second, first), 6, 0))


def shrink(x, op):
    x = op(x[:16], x[16:]).astype(jnp.float32)
    return op(x[:8], x[8:])


def page_kernel(
    seqs, heads, lengths_hbm, keys, query, bounds_in, mean, score,
    lengths, buf, bounds, code, code_in, query_in, low_wide, high_wide, query_wide,
    key_sem, bounds_send, bounds_recv, code_send, code_recv, query_send, query_recv, query_own, length_sem,
):
    head = lax.axis_index("head")
    seq = lax.axis_index("seq")
    ratio = seqs // heads
    pages = keys.shape[1]
    tall = keys.shape[2]
    width = tall // PAGE
    lanes = keys.shape[3]
    block = buf.shape[1]
    blocks = pages // block
    steps = seqs * blocks
    rows = block * width
    group = min(8, block)
    chunk = min(32, block)
    owner = seq // ratio
    part = lax.rem(seq, ratio)
    mine = owner == head

    barrier = pltpu.get_barrier_semaphore()

    def greet(i, carry):
        source_head = i // ratio
        source_seq = head * ratio + lax.rem(i, ratio)

        @pl.when(jnp.logical_or(source_head != head, source_seq != seq))
        def _():
            pl.semaphore_signal(barrier, inc=1, device_id=(source_head, source_seq), device_id_type=MESH)

        return carry

    lax.fori_loop(0, seqs, greet, 0)
    for i in range(1, heads):
        pl.semaphore_signal(barrier, inc=1, device_id=(lax.rem(head + i, heads), seq), device_id_type=MESH)

    def dest_of(step):
        pairs = seqs // 2
        half = pairs // 2
        k = step // blocks
        pair = k // 2
        own = seq // 2
        lower = own < half
        place = jnp.where(lower, own, pairs - 1 - own)
        near = jnp.where(place < half // 2, pairs - 1 - pair, pair - half)
        other = jnp.where(pair < half, pairs - 1 - pair, near)
        return 2 * jnp.where(lower, other, pairs - 1 - other) + lax.rem(seq + k, 2)

    def fetch(step):
        slot = lax.rem(step, SLOTS)
        at = pl.ds(lax.rem(step, blocks) * block, block)
        return pltpu.make_async_copy(keys.at[dest_of(step), at], buf.at[slot], key_sem.at[slot])

    own_lengths = pltpu.make_async_copy(lengths_hbm, lengths, length_sem)
    own_lengths.start()
    for step in range(min(SLOTS - 1, steps)):
        fetch(jnp.int32(step)).start()
    own_query = pltpu.make_async_copy(query, query_in.at[head], query_own)
    own_query.start()

    def query_copy(i, target):
        return pltpu.make_async_remote_copy(
            src_ref=query, dst_ref=query_in.at[head], send_sem=query_send.at[i], recv_sem=query_recv.at[i],
            device_id=(target, seq), device_id_type=MESH,
        )

    index = head * ratio + part

    def landing(step):
        return pl.ds(pl.multiple_of((part * pages + lax.rem(step, blocks) * block) * width, rows), rows)

    def inside_of(step):
        return pl.ds(pl.multiple_of(lax.rem(step, blocks) * rows, rows), rows)

    def whole_bounds(step):
        return pltpu.make_async_remote_copy(
            src_ref=bounds.at[step // blocks],
            dst_ref=bounds_in.at[head, part],
            send_sem=bounds_send.at[step // blocks],
            recv_sem=bounds_recv.at[index],
            device_id=(owner, dest_of(step)),
            device_id_type=MESH,
        )

    def block_bounds(step):
        return pltpu.make_async_remote_copy(
            src_ref=bounds.at[step // blocks, :, inside_of(step)],
            dst_ref=bounds_in.at[head, part, :, inside_of(step)],
            send_sem=bounds_send.at[step // blocks],
            recv_sem=bounds_recv.at[index],
            device_id=(owner, dest_of(step)),
            device_id_type=MESH,
        )

    def block_code(step):
        return pltpu.make_async_remote_copy(
            src_ref=code.at[step // blocks, inside_of(step)],
            dst_ref=code_in.at[head, landing(step)],
            send_sem=code_send.at[step // blocks],
            recv_sem=code_recv.at[index],
            device_id=(owner, dest_of(step)),
            device_id_type=MESH,
        )

    def whole_code(step):
        return pltpu.make_async_remote_copy(
            src_ref=code.at[step // blocks],
            dst_ref=code_in.at[head, pl.ds(pl.multiple_of(part * pages * width, pages * width), pages * width)],
            send_sem=code_send.at[step // blocks],
            recv_sem=code_recv.at[index],
            device_id=(owner, dest_of(step)),
            device_id_type=MESH,
        )

    adder_row = lax.broadcasted_iota(jnp.int32, (group * width, group * tall), 0)
    adder_column = lax.broadcasted_iota(jnp.int32, (group * width, group * tall), 1)
    adder = jnp.logical_and(
        adder_row // width == adder_column // tall, lax.rem(adder_row, width) == lax.rem(adder_column, width)
    ).astype(jnp.bfloat16)
    adder_token = (adder_column // width).astype(jnp.int16)
    eight = lax.broadcasted_iota(jnp.int32, (8, lanes), 0)
    page_of = lax.broadcasted_iota(jnp.int32, (chunk * width, lanes), 0) // width
    token_of = (lax.broadcasted_iota(jnp.int32, (tall, lanes), 0) // width).astype(jnp.int16)
    above = jnp.full((tall, lanes), jnp.inf, jnp.bfloat16)
    own_lengths.wait()

    def work(step, carry):
        @pl.when(step + SLOTS - 1 < steps)
        def _():
            fetch(step + SLOTS - 1).start()

        slot = lax.rem(step, SLOTS)
        dest = dest_of(step)
        fetch(step).wait()
        limit = jnp.clip(lengths[dest] - (seq * pages + lax.rem(step, blocks) * block) * PAGE, 0, block * PAGE)

        def piece(c, carry):
            small, large, total = [], [], []
            for g in range(chunk // group):
                start = c * chunk + g * group
                left = limit - start * PAGE
                lows, highs = [], []
                for p in range(group):
                    x = buf[slot, start + p]
                    keep = token_of < jnp.clip(left - p * PAGE, 0, PAGE).astype(jnp.int16)
                    lows.append(shrink(jnp.where(keep, x, above), jnp.minimum))
                    highs.append(shrink(jnp.where(keep, x, -above), jnp.maximum))
                for p in range(0, group, 4):
                    small.append(gather(lows[p:p + 4], jnp.minimum, eight))
                    large.append(gather(highs[p:p + 4], jnp.maximum, eight))
                x = buf[slot, pl.ds(start, group)].reshape(group * tall, lanes)
                counted = adder_token < jnp.clip(left, 0, group * PAGE).astype(jnp.int16)
                weight = jnp.where(counted, adder, jnp.zeros_like(adder))
                total.append(jnp.dot(weight, x, preferred_element_type=jnp.float32))
            live = (page_of + c * chunk) * PAGE < limit
            small = jnp.where(live, jnp.concatenate(small, axis=0), 0.0)
            large = jnp.where(live, jnp.concatenate(large, axis=0), 0.0)
            total = jnp.concatenate(total, axis=0)
            bound = jnp.maximum(jnp.abs(small), jnp.abs(large))
            share = jnp.abs(total) / (PAGE * jnp.where(bound > 0.0, bound, 1.0))
            level = jnp.log2(jnp.maximum(share, 1e-30)) * (TOP / SPAN) + TOP
            level = jnp.clip(level + 0.5, 0.0, TOP)
            level = jnp.where(total < 0.0, -level, level)
            at = pl.ds(pl.multiple_of(lax.rem(step, blocks) * rows + c * chunk * width, chunk * width), chunk * width)
            bounds[step // blocks, 0, at, :] = small.astype(bounds.dtype)
            bounds[step // blocks, 1, at, :] = large.astype(bounds.dtype)
            code[step // blocks, at, :] = level.astype(jnp.int32).astype(jnp.int16)
            return carry

        lax.fori_loop(0, block // chunk, piece, 0)

        @pl.when(step == 0)
        def _():
            pl.semaphore_wait(barrier, seqs - jnp.where(mine, 1, 0) + heads - 1)

        itself = jnp.logical_and(mine, dest == seq)

        @pl.when(itself)
        def _():
            bounds_in[head, part, :, inside_of(step)] = bounds[step // blocks, :, inside_of(step)]
            code_in[head, landing(step)] = code[step // blocks, inside_of(step)]

        @pl.when(jnp.logical_and(jnp.logical_not(itself), step < blocks))
        def _():
            block_bounds(step).start()
            block_code(step).start()

        complete = jnp.logical_and(step >= blocks, lax.rem(step, blocks) == blocks - 1)

        @pl.when(jnp.logical_and(jnp.logical_not(itself), complete))
        def _():
            whole_bounds(step).start()
            whole_code(step).start()

        return carry

    lax.fori_loop(0, steps, work, 0)

    for i in range(heads - 1):
        query_copy(i, lax.rem(head + i + 1, heads)).start()
    own_query.wait()
    for i in range(heads - 1):
        query_copy(i, lax.rem(head + i + 1, heads)).wait()

    owned = pages * ratio
    shared = query_in.shape[1] // width
    query_wide[...] = query_in[...].reshape(query_wide.shape).astype(jnp.float32)
    unit = min(max(LANE, pages), owned)
    unit_rows = unit * width
    each = unit // pages
    message = pages * width
    slab = min(256, rows)
    parts = message // slab
    limit = lengths[seq] - head * owned * PAGE
    row_page = lax.broadcasted_iota(jnp.int32, (slab, lanes), 0) // width

    dims = (((1,), (1,)), ((), ()))

    def finish(i, carry):
        u = i
        if each == 1:
            u = lax.rem(i + seq, ratio)
        across = pl.ds(pl.multiple_of(u * unit, unit), unit)

        def elsewhere(source_head, source_part):
            return jnp.logical_or(source_head != head, head * ratio + source_part != seq)

        def spread(source_head, carry):
            for j in range(each):
                source_part = u * each + j

                @pl.when(elsewhere(source_head, source_part))
                def _():
                    pltpu.make_async_remote_copy(
                        src_ref=bounds.at[0],
                        dst_ref=bounds_in.at[source_head, source_part],
                        send_sem=bounds_send.at[0],
                        recv_sem=bounds_recv.at[source_head * ratio + source_part],
                        device_id=(source_head, head * ratio + source_part),
                        device_id_type=MESH,
                    ).wait_recv()

            def widen(c, carry):
                inside = pl.ds(pl.multiple_of(c * slab, slab), slab)
                at = pl.ds(pl.multiple_of(u * unit_rows + c * slab, slab), slab)
                local = pl.ds(pl.multiple_of(lax.rem(c, parts) * slab, slab), slab)
                small = bounds_in[source_head, u * each + c // parts, 0, local, :].astype(jnp.float32)
                large = bounds_in[source_head, u * each + c // parts, 1, local, :].astype(jnp.float32)
                low_wide[inside, :] = small
                high_wide[inside, :] = large
                first = u * unit + c * (slab // width)
                count = jnp.clip(limit - (first + row_page) * PAGE, 1, PAGE).astype(jnp.float32)
                mean[source_head, at, :] = jnp.maximum(jnp.abs(small), jnp.abs(large)) * PAGE / count
                return carry

            lax.fori_loop(0, unit_rows // slab, widen, 0)
            for j in range(width):
                at = pl.ds(pl.multiple_of((source_head * width + j) * shared, shared), shared)
                q = query_wide[at, :]
                up = high_wide[pl.ds(j, unit, stride=width), :].astype(jnp.bfloat16)
                down = low_wide[pl.ds(j, unit, stride=width), :].astype(jnp.bfloat16)
                both = lax.dot_general(
                    jnp.maximum(q, 0.0).astype(jnp.bfloat16), up, dims, preferred_element_type=jnp.float32
                ) + lax.dot_general(
                    jnp.minimum(q, 0.0).astype(jnp.bfloat16), down, dims, preferred_element_type=jnp.float32
                )
                score[at, across] = both * lanes ** (-0.5)
            return carry

        def average(n, carry):
            source_head = lax.rem(n, heads)
            source_part = u * each + n // heads

            @pl.when(elsewhere(source_head, source_part))
            def _():
                pltpu.make_async_remote_copy(
                    src_ref=code.at[0],
                    dst_ref=code_in.at[source_head, pl.ds(pl.multiple_of(source_part * message, message), message)],
                    send_sem=code_send.at[0],
                    recv_sem=code_recv.at[source_head * ratio + source_part],
                    device_id=(source_head, head * ratio + source_part),
                    device_id_type=MESH,
                ).wait_recv()

            def decode(c, carry):
                at = pl.ds(pl.multiple_of(source_part * message + c * slab, slab), slab)
                level = code_in[source_head, at, :].astype(jnp.int32).astype(jnp.float32)
                share = jnp.exp2((jnp.abs(level) - TOP) * (SPAN / TOP))
                share = jnp.where(level == 0.0, 0.0, jnp.where(level < 0.0, -share, share))
                mean[source_head, at, :] = mean[source_head, at, :] * share
                return carry

            lax.fori_loop(0, message // slab, decode, 0)
            return carry

        lax.fori_loop(0, heads, spread, 0)
        lax.fori_loop(0, heads * each, average, 0)
        return carry

    lax.fori_loop(0, owned // unit, finish, 0)

    def sent(step, carry):
        @pl.when(jnp.logical_not(jnp.logical_and(mine, dest_of(step) == seq)))
        def _():
            @pl.when(lax.rem(step, blocks) == 0)
            def _():
                whole_bounds(step).wait_send()
                whole_code(step).wait_send()

        return carry

    lax.fori_loop(0, steps, sent, 0)


def store_kernel(bounds, mean, score, low_out, high_out, mean_out, score_out, sem):
    copies = []
    for head in range(bounds.shape[0]):
        copies.append(pltpu.make_async_copy(mean.at[head], mean_out.at[:, :, head], sem.at[0, head]))
        for k, target in ((0, low_out), (1, high_out)):
            copies.append(pltpu.make_async_copy(bounds.at[head, :, k], target.at[:, :, head], sem.at[1 + k, head]))
    copies.append(pltpu.make_async_copy(score, score_out, sem.at[3, 0]))
    for copy in copies:
        copy.start()
    for copy in copies:
        copy.wait()


def local_step(heads, seqs, cached_keys, queries, seq_lengths):
    seq_count, tokens, width, lanes = cached_keys.shape
    pages = tokens // PAGE
    owned = pages * seqs // heads
    local_q = queries.shape[1]
    kv_heads = heads * width
    count_q = heads * local_q
    block = min(BLOCK, pages)
    blocks = pages // block
    unit = min(max(LANE, pages), owned)
    tall = PAGE * width
    keys = cached_keys.reshape(seq_count, pages, tall, lanes)
    vmem = pl.BlockSpec(memory_space=pltpu.VMEM)
    hbm = pl.BlockSpec(memory_space=pltpu.HBM)
    shape = (heads, owned * width, lanes)
    ratio = seqs // heads
    message = pages * width
    bounds, mean, score = pl.pallas_call(
        functools.partial(page_kernel, seqs, heads),
        out_shape=(
            pltpu.VMEM((heads, ratio, 2, message, lanes), jnp.bfloat16),
            pltpu.VMEM(shape, jnp.float32),
            pltpu.VMEM((count_q, owned), jnp.float32),
        ),
        in_specs=[hbm] * 3,
        out_specs=(vmem,) * 3,
        scratch_shapes=[
            pltpu.SMEM((seq_count,), jnp.int32),
            pltpu.VMEM((SLOTS, block, tall, lanes), jnp.bfloat16),
            pltpu.VMEM((seqs, 2, message, lanes), jnp.bfloat16),
            pltpu.VMEM((seqs, message, lanes), jnp.int16),
            pltpu.VMEM(shape, jnp.int16),
            pltpu.VMEM((heads, local_q, lanes), jnp.bfloat16),
            pltpu.VMEM((unit * width, lanes), jnp.float32),
            pltpu.VMEM((unit * width, lanes), jnp.float32),
            pltpu.VMEM((count_q, lanes), jnp.float32),
            pltpu.SemaphoreType.DMA((SLOTS,)),
            pltpu.SemaphoreType.DMA((seqs,)),
            pltpu.SemaphoreType.DMA((seqs,)),
            pltpu.SemaphoreType.DMA((seqs,)),
            pltpu.SemaphoreType.DMA((seqs,)),
            pltpu.SemaphoreType.DMA((heads - 1,)),
            pltpu.SemaphoreType.DMA((heads - 1,)),
            pltpu.SemaphoreType.DMA,
            pltpu.SemaphoreType.DMA,
        ],
        compiler_params=pltpu.CompilerParams(collective_id=0, has_side_effects=True, vmem_limit_bytes=24 << 20),
        name="page_exchange",
    )(
        pltpu.with_memory_space_constraint(seq_lengths, pltpu.HBM),
        pltpu.with_memory_space_constraint(keys, pltpu.HBM),
        pltpu.with_memory_space_constraint(queries.reshape(local_q, lanes), pltpu.HBM),
    )
    whole = (ratio, pages, heads, width, lanes)
    low, high, mean, score = pl.pallas_call(
        store_kernel,
        out_shape=(
            jax.ShapeDtypeStruct(whole, jnp.bfloat16),
            jax.ShapeDtypeStruct(whole, jnp.bfloat16),
            jax.ShapeDtypeStruct(whole, jnp.float32),
            jax.ShapeDtypeStruct((count_q, owned), jnp.float32),
        ),
        in_specs=[vmem] * 3,
        out_specs=(hbm,) * 4,
        scratch_shapes=[pltpu.SemaphoreType.DMA((4, heads))],
        compiler_params=pltpu.CompilerParams(vmem_limit_bytes=16 << 20),
        name="page_store",
    )(
        bounds.reshape(heads, ratio, 2, pages, width, lanes),
        mean.reshape(heads, ratio, pages, width, lanes),
        score,
    )
    final = (1, owned, kv_heads, lanes)
    return low.reshape(final), high.reshape(final), mean.reshape(final), score.reshape(1, count_q, owned)


def solution(mesh):
    return jax.shard_map(
        functools.partial(local_step, mesh.shape["head"], mesh.shape["seq"]),
        mesh=mesh,
        in_specs=(P(None, "seq", "head", None), P("seq", "head", None), P()),
        out_specs=(
            P("seq", "head", None, None),
            P("seq", "head", None, None),
            P("seq", "head", None, None),
            P("seq", None, "head"),
        ),
        check_vma=False,
    )
```
